32 devices in a mesh: seq: 8 (over z, y), head: 4 (over x, core).
Axes of the slice: x: 2, y: 2, z: 4, core: 2. Of those that a mesh axis runs over, the one named last changes fastest.
Arguments:
- queries: bfloat16 [2048, 2048], P(('seq', 'head')), may hold values from -200 to 200
- keys: bfloat16 [2048, 2048], P(('seq', 'head')), may hold values from -15 to 15
- values: bfloat16 [2048, 2048], P(('seq', 'head')), may hold values from -6 to 6
- random_blocks: int32 [32, 16, 3], P('seq', 'head'), may hold values from 0 to 31, as said below
- global_blocks: int32 [2], replicated, may hold values from 0 to 31, as said below
Outputs:
- attention: float32 [2048, 2048], P('seq', 'head')
The draws below stay inside these ranges and needn't reach their ends.
Inputs may be any that keep to these rules, and one draw needn't show every extreme that they name: `random_blocks`: over the 4 query blocks and 4 heads of one device (one index of seq and one of head), at most 9 entries name blocks of any one shard of 4 consecutive blocks; in every draw some device names exactly 9 blocks of one shard. Entries may repeat and may fall on the window or on a global block. `global_blocks`: two different block numbers; one of them is 31.
All inputs are finite; a program needn't handle non-finite values.
Results may differ from the reference program's by a relative error of at most 0.0023.
Values may be sent and summed in bfloat16 or wider, within the bound.
A program may use at most 128 MiB of HBM per device.

```python
import math
import jax
import jax.numpy as jnp
from jax import lax

HEADS = 16
HEAD_DIM = 128
BLK = 64
RAND = 3
GLOB = 2
BLK_DEV = 4
HEADS_DEV = 4
NB = 32
TOKENS = 2048
CAP = 9


def draw_pair(key):
    base_key = jax.random.fold_in(key, 101)
    query_key, key_key = jax.random.split(base_key, 2)
    dims = (TOKENS, HEADS * HEAD_DIM)
    query_draw = 2.0 * jnp.clip(jax.random.normal(query_key, dims, jnp.float32), -6.0, 6.0)
    key_draw = jnp.clip(jax.random.normal(key_key, dims, jnp.float32), -6.0, 6.0)
    return (query_draw, key_draw)


def draw_queries(key, part):
    return draw_pair(key)[0].astype(jnp.bfloat16)


def draw_keys(key, part):
    return draw_pair(key)[1].astype(jnp.bfloat16)


def draw_random_blocks(key, part):
    base_key = jax.random.fold_in(key, 202)
    seq_count = NB // BLK_DEV
    head_groups = HEADS // HEADS_DEV
    per_device = BLK_DEV * HEADS_DEV * RAND

    def one_device(device_key):
        perm_key, favor_key, order_key, block_key = jax.random.split(device_key, 4)
        owners = jnp.tile(jnp.arange(seq_count, dtype=jnp.int32), CAP)
        favored = jax.random.randint(favor_key, (), 0, seq_count)
        shuffled = jax.random.permutation(perm_key, seq_count * CAP).astype(jnp.int32)
        ranking = jnp.where(owners == favored, -1, shuffled)
        chosen = owners[jnp.argsort(ranking, stable=True)][:per_device]
        chosen = chosen[jax.random.permutation(order_key, per_device)]
        offsets = jax.random.randint(block_key, (per_device,), 0, BLK_DEV)
        return (chosen * BLK_DEV + offsets).astype(jnp.int32).reshape(BLK_DEV, HEADS_DEV, RAND)
    device_keys = jax.random.split(base_key, seq_count * head_groups)
    drawn = jax.vmap(one_device)(device_keys)
    drawn = drawn.reshape(seq_count, head_groups, BLK_DEV, HEADS_DEV, RAND).transpose(0, 2, 1, 3, 4)
    return drawn.reshape(NB, HEADS, RAND)


def draw_global_blocks(key, part):
    base_key = jax.random.fold_in(key, 303)
    other_key, place_key = jax.random.split(base_key, 2)
    other = jax.random.randint(other_key, (), 0, NB - 1).astype(jnp.int32)
    last = jnp.array(NB - 1, jnp.int32)
    place = jax.random.randint(place_key, (), 0, 2)
    first_entry = jnp.where(place == 0, last, other)
    second_entry = jnp.where(place == 0, other, last)
    return jnp.stack([first_entry, second_entry]).astype(jnp.int32)


def level_of(rng, extent, cuts, least, high):
    loudness, own = 1.0, jax.random.fold_in(rng, 6)
    for dim, shards_of in cuts:
        steps = jnp.exp(jax.random.uniform(jax.random.fold_in(own, dim), (shards_of,), jnp.float32, least / len(cuts), high / len(cuts)))
        loudness = loudness * jnp.repeat(steps, extent[dim] // shards_of).reshape([-1 if axis == dim else 1 for axis in range(len(extent))])
    return loudness


def scatter_about(key, extent, deviation, most, pieces=(), held_as=jnp.bfloat16):
    entries = deviation * jax.random.normal(key, extent, jnp.float32)
    if pieces:
        entries = entries * level_of(key, extent, pieces, -0.22, 0.18)
    return jnp.clip(entries, -most, most).astype(held_as)


def setup_inputs(seed: int = 0) -> dict:
    key_of = jax.random.split(jax.random.key(seed), 6)
    queries = draw_queries(jax.random.fold_in(key_of[5], 71), 0)
    keys = draw_keys(jax.random.fold_in(key_of[5], 71), 0)
    values = scatter_about(key_of[2], (TOKENS, HEADS * HEAD_DIM), 1.0, 6.0, ((0, 32),))
    random_blocks = draw_random_blocks(jax.random.fold_in(key_of[5], 71), 0)
    global_blocks = draw_global_blocks(jax.random.fold_in(key_of[5], 71), 0)
    return dict(queries=queries, keys=keys, values=values, random_blocks=random_blocks, global_blocks=global_blocks)


MASKED = -1e+30

def attend(scores, value_set):
    peaks = lax.optimization_barrier(jnp.max(scores, axis=-1, keepdims=True))
    powers = jnp.exp(scores - peaks)
    totals = lax.optimization_barrier(jnp.sum(powers, axis=-1, keepdims=True))
    weights = lax.optimization_barrier(powers.astype(jnp.bfloat16)).astype(jnp.float32)
    return jnp.einsum('hqk,hkd->hqd', weights, value_set.astype(jnp.float32)) / totals

def reference(queries, keys, values, random_blocks, global_blocks):
    score_scale = 1.0 / math.sqrt(HEAD_DIM)
    block_shape = (NB, BLK, HEADS, HEAD_DIM)
    query_blocks = queries.reshape(block_shape)
    key_blocks = keys.reshape(block_shape)
    value_blocks = values.reshape(block_shape)
    head_ids = jnp.arange(HEADS, dtype=jnp.int32)[:, None]

    def gather_blocks(source_table, block_id, rand_ids):
        near_ids = jnp.clip(block_id + jnp.arange(-1, 2, dtype=jnp.int32), 0, NB - 1)
        window = jnp.transpose(source_table[near_ids], (2, 0, 1, 3))
        global_part = jnp.transpose(source_table[global_blocks], (2, 0, 1, 3))
        random_part = source_table[rand_ids, :, head_ids, :]
        joined = jnp.concatenate([window, global_part, random_part], axis=1)
        return joined.reshape(HEADS, (3 + GLOB + RAND) * BLK, HEAD_DIM)

    def sparse_row(block_id):
        rand_ids = random_blocks[block_id]
        near_ids = block_id + jnp.arange(-1, 2, dtype=jnp.int32)
        in_range = (near_ids >= 0) & (near_ids < NB)
        keep_mask = jnp.concatenate([jnp.repeat(in_range, BLK), jnp.ones(((GLOB + RAND) * BLK,), dtype=bool)])
        key_set = gather_blocks(key_blocks, block_id, rand_ids).astype(jnp.float32)
        value_set = gather_blocks(value_blocks, block_id, rand_ids)
        query_set = jnp.transpose(query_blocks[block_id], (1, 0, 2)).astype(jnp.float32)
        scores = jnp.einsum('hqd,hkd->hqk', query_set, key_set) * score_scale
        scores = jnp.where(keep_mask[None, None, :], scores, MASKED)
        return attend(scores, value_set)
    sparse = lax.map(sparse_row, jnp.arange(NB, dtype=jnp.int32))
    sparse = jnp.transpose(sparse, (0, 2, 1, 3))
    global_query = query_blocks[global_blocks]
    flat_keys = keys.reshape(TOKENS, HEADS, HEAD_DIM)
    flat_values = values.reshape(TOKENS, HEADS, HEAD_DIM)

    def full_head(head_id):
        query_set = jnp.take(global_query, head_id, axis=2).reshape(GLOB * BLK, HEAD_DIM)
        key_set = jnp.take(flat_keys, head_id, axis=1)
        value_set = jnp.take(flat_values, head_id, axis=1)
        scores = jnp.dot(query_set, key_set.T, preferred_element_type=jnp.float32) * score_scale
        return attend(scores[None], value_set[None])[0]
    full_rows = lax.map(full_head, jnp.arange(HEADS, dtype=jnp.int32))
    full_rows = jnp.transpose(full_rows.reshape(HEADS, GLOB, BLK, HEAD_DIM), (1, 2, 0, 3))
    attention = sparse.at[global_blocks].set(full_rows)
    return attention.reshape(TOKENS, HEADS * HEAD_DIM)
```

```python
import functools
import math

import jax
import jax.numpy as jnp
from jax import lax
from jax.experimental import pallas as pl
from jax.experimental.pallas import tpu as pltpu
from jax.sharding import PartitionSpec as P

HEAD_DIM = 128
BLK = 64


MASKED = -1e30


def extended(block, sides, width):
    for axis, dim in sides:
        count = lax.axis_size(axis)
        forward = [(i, i + 1) for i in range(count - 1)]
        backward = [(target, source) for source, target in forward]
        low = lax.ppermute(
            lax.slice_in_dim(block, block.shape[dim] - width, None, axis=dim), axis, forward
        )
        high = lax.ppermute(lax.slice_in_dim(block, 0, width, axis=dim), axis, backward)
        block = jnp.concatenate([low, block, high], axis=dim)
    return block


def combined_all(value, axis, join):
    pieces = jax.tree.map(lambda part: lax.all_gather(part, axis), value)
    head = jax.tree.map(lambda part: part[0], pieces)
    tail = jax.tree.map(lambda part: part[1:], pieces)
    so_far, _ = lax.scan(lambda so_far, slab: (join(so_far, slab), None), head, tail)
    return so_far


def merge_parts(former, latter):
    peaks = jnp.maximum(former[0], latter[0])
    former_fade = jnp.exp(former[0] - peaks)
    latter_fade = jnp.exp(latter[0] - peaks)
    return (
        peaks,
        former[1] * former_fade + latter[1] * latter_fade,
        former[2] * former_fade[..., None] + latter[2] * latter_fade[..., None],
    )


def soft_parts(scores):
    peaks = jnp.max(scores, axis=(-2, -1))
    powers = jnp.exp(scores - peaks[..., None, None])
    return (peaks, jnp.sum(powers, axis=(-2, -1)), powers.astype(jnp.bfloat16))


def make_requests(rand_lists, seq_count, capacity):
    blk_dev, heads_dev, rand_count = rand_lists.shape
    flat_list = rand_lists.reshape(-1)
    owners = flat_list // blk_dev
    head_ids = jnp.broadcast_to(
        jnp.arange(heads_dev, dtype=jnp.int32)[None, :, None], rand_lists.shape
    ).reshape(-1)
    item_ids = flat_list % blk_dev * heads_dev + head_ids
    position = jnp.arange(flat_list.shape[0], dtype=jnp.int32)
    earlier = (owners[:, None] == owners[None, :]) & (position[None, :] < position[:, None])
    slot_ids = owners * capacity + jnp.sum(earlier.astype(jnp.int32), axis=1)
    requests = jnp.zeros((seq_count * capacity,), jnp.int32).at[slot_ids].set(item_ids)
    sources = jnp.zeros((seq_count * capacity,), jnp.int32).at[slot_ids].set(position)
    return (requests.reshape(seq_count, capacity), slot_ids, sources)


def exchanged(queries, keys, values, random_blocks, global_blocks):
    seq_count = lax.axis_size("seq")
    seq_index = lax.axis_index("seq")
    query_rows, key_rows, value_rows = (
        lax.all_to_all(queries, "head", split_axis=1, concat_axis=0, tiled=True),
        lax.all_to_all(keys, "head", split_axis=1, concat_axis=0, tiled=True),
        lax.all_to_all(values, "head", split_axis=1, concat_axis=0, tiled=True),
    )
    tokens = query_rows.shape[0]
    blk_dev = tokens // BLK
    heads_dev = query_rows.shape[1] // HEAD_DIM
    rand_count = random_blocks.shape[2]
    glob_count = global_blocks.shape[0]
    total_blocks = blk_dev * seq_count
    first_block = seq_index * blk_dev
    capacity = (blk_dev * heads_dev * rand_count * 3 // 2 + seq_count - 1) // seq_count
    score_scale = 1.0 / math.sqrt(HEAD_DIM)
    shape_four = (blk_dev, BLK, heads_dev, HEAD_DIM)
    query_four = query_rows.reshape(shape_four)
    key_four = key_rows.reshape(shape_four)
    value_four = value_rows.reshape(shape_four)
    paired = jnp.stack([key_rows, value_rows])
    padded = extended(paired, (("seq", 1),), BLK)
    padded = padded.reshape(2, blk_dev + 2, BLK, heads_dev, HEAD_DIM)
    window = jnp.stack([padded[:, offset : offset + blk_dev] for offset in range(3)], axis=2)
    near_ids = (
        first_block
        + jnp.arange(blk_dev, dtype=jnp.int32)[:, None]
        + jnp.arange(-1, 2, dtype=jnp.int32)[None, :]
    )
    inside = (near_ids >= 0) & (near_ids < total_blocks)
    stacked = jnp.stack([query_rows, key_rows, value_rows]).reshape(
        3, blk_dev, BLK, heads_dev * HEAD_DIM
    )
    owned_mask = global_blocks // blk_dev == seq_index
    local_ids = jnp.where(owned_mask, global_blocks - first_block, 0)
    picked = (
        jnp.take(stacked, local_ids, axis=1).astype(jnp.float32)
        * owned_mask.astype(jnp.float32)[None, :, None, None]
    )
    glob_rows = lax.psum(picked, "seq").astype(jnp.bfloat16)
    glob_rows = glob_rows.reshape(3, glob_count, BLK, heads_dev, HEAD_DIM)
    requests, slot_ids, sources = make_requests(random_blocks, seq_count, capacity)
    incoming = lax.all_to_all(requests, "seq", split_axis=0, concat_axis=0, tiled=True)

    def by_block(row_data):
        return (
            row_data.reshape(shape_four)
            .transpose(0, 2, 1, 3)
            .reshape(blk_dev * heads_dev, BLK, HEAD_DIM)
        )

    pair_blocks = jnp.stack([by_block(key_rows), by_block(value_rows)], axis=1)
    served = pair_blocks[incoming]
    key_win, value_win = (window[0], window[1])
    win_scores = (
        jnp.einsum("jqhd,jwkhd->jhqwk", query_four, key_win, preferred_element_type=jnp.float32)
        * score_scale
    )
    win_scores = jnp.where(inside[:, None, None, :, None], win_scores, MASKED)
    glob_scores = (
        jnp.einsum("jqhd,gkhd->jhqgk", query_four, glob_rows[1], preferred_element_type=jnp.float32)
        * score_scale
    )
    split_at = 3 + glob_count
    arrived_pairs = lax.all_to_all(served, "seq", split_axis=0, concat_axis=0, tiled=True)
    tail = arrived_pairs.shape[2:]
    rand_pairs = arrived_pairs.reshape((seq_count * capacity,) + tail)[slot_ids].reshape(
        (blk_dev, heads_dev, rand_count) + tail
    )
    rand_scores = (
        jnp.einsum(
            "jqhd,jhrkd->jhqrk",
            query_four,
            rand_pairs[:, :, :, 0],
            preferred_element_type=jnp.float32,
        )
        * score_scale
    )
    peaks, totals, weights = soft_parts(
        jnp.concatenate([win_scores, glob_scores, rand_scores], axis=3)
    )
    sums_all = jnp.einsum(
        "jhqwk,jwkhd->jhqd", weights[:, :, :, 0:3], value_win, preferred_element_type=jnp.float32
    )
    sums_all = sums_all + jnp.einsum(
        "jhqgk,gkhd->jhqd",
        weights[:, :, :, 3:split_at],
        glob_rows[2],
        preferred_element_type=jnp.float32,
    )
    sums_all = sums_all + jnp.einsum(
        "jhqrk,jhrkd->jhqd",
        weights[:, :, :, split_at:],
        rand_pairs[:, :, :, 1],
        preferred_element_type=jnp.float32,
    )
    running = (peaks, totals, sums_all)
    sparse_out = (running[2] / running[1][..., None]).transpose(0, 2, 1, 3)
    full_scores = (
        jnp.einsum("gqhd,jkhd->hgqjk", glob_rows[0], key_four, preferred_element_type=jnp.float32)
        * score_scale
    )
    full_peaks, full_totals, full_weights = soft_parts(full_scores)
    full_sum = jnp.einsum(
        "hgqjk,jkhd->hgqd", full_weights, value_four, preferred_element_type=jnp.float32
    )
    merged = combined_all((full_peaks, full_totals, full_sum), "seq", merge_parts)
    glob_out = (merged[2] / merged[1][..., None]).transpose(1, 2, 0, 3)
    block_ids = first_block + jnp.arange(blk_dev, dtype=jnp.int32)
    result = sparse_out
    for glob_id in range(glob_count):
        matches = (block_ids == global_blocks[glob_id])[:, None, None, None]
        result = jnp.where(matches, glob_out[glob_id][None], result)
    return result.reshape(tokens, heads_dev * HEAD_DIM)


GATHER_LIMIT = 16 * 2**20


def gathered_kernel(
    seq_count, head_count, rand_count, glob_count,
    q_hbm, k_hbm, v_hbm, rand_ref, glob_ref, out_ref,
    pool, q_all, stage, q_stage, listed, peak_ref, total_ref, acc_ref,
    local_sem, send_sem, recv_sem, q_send_sem, q_recv_sem,
):
    seq = lax.axis_index("seq")
    head = lax.axis_index("head")
    depth = seq_count // 2
    z, y = seq // 2, seq % 2
    rows, width = q_all.shape[1], q_all.shape[2]
    heads_dev = width // HEAD_DIM
    tokens = head_count * rows
    classes = head_count

    def lane(k):
        return ((head // 2 + k // 2) % (head_count // 2)) * 2 + (head % 2 + k % 2) % 2

    def shard(dz, dy):
        return ((z + dz) % depth) * 2 + (y + dy) % 2

    def spot(dz, dy, k):
        return shard(dz, dy) * head_count + lane(k)

    loads = []
    for k in range(classes):
        cols = pl.ds(pl.multiple_of(lane(k) * width, 128), width)
        target = pool.at[spot(0, 0, 0)] if k == 0 else stage.at[k - 1]
        q_target = q_all.at[head] if k == 0 else q_stage.at[k - 1]
        trio = []
        for n, (source, dest) in enumerate(
            ((k_hbm, target.at[0]), (v_hbm, target.at[1]), (q_hbm, q_target))
        ):
            trio.append(pltpu.make_async_copy(source.at[:, cols], dest, local_sem.at[k * 3 + n]))
        loads.append(trio)
    for n in range(3):
        for trio in loads if n == 2 else ():
            trio[n].start()
        for trio in loads if n == 0 else ():
            trio[0].start()
            trio[1].start()

    barrier = pltpu.get_barrier_semaphore()
    friends = [{"seq": seq, "head": lane(k)} for k in range(1, classes)]
    friends.append({"seq": shard(0, 1), "head": head})
    friends.append({"seq": shard(1, 0), "head": head})
    friends.append({"seq": shard(-1, 0), "head": head})
    for friend in friends:
        pl.semaphore_signal(barrier, inc=1, device_id=friend, device_id_type=pl.DeviceIdType.MESH)

    query_block = seq * (tokens // BLK) + lax.broadcasted_iota(jnp.int32, (1, tokens), 1) // BLK
    local_block = lax.broadcasted_iota(jnp.int32, (1, tokens), 1) // BLK
    for hd in range(heads_dev):
        for r in range(rand_count):
            names = jnp.zeros((1, tokens), jnp.int32)
            for b in range(tokens // BLK):
                names = jnp.where(local_block == b, rand_ref[b, hd, r], names)
            listed[pl.ds(hd * rand_count + r, 1), :] = names
    is_glob = query_block == glob_ref[0]
    for g in range(1, glob_count):
        is_glob = is_glob | (query_block == glob_ref[g])
    glob_row = jnp.where(is_glob, 1, 0)
    peak_ref[...] = jnp.full_like(peak_ref, MASKED)
    total_ref[...] = jnp.zeros_like(total_ref)
    acc_ref[...] = jnp.zeros_like(acc_ref)

    for trio in loads:
        trio[0].wait()
        trio[1].wait()
    for trio in loads:
        trio[2].wait()
    pl.semaphore_wait(barrier, len(friends))

    pending = []
    landed = {(0, 0, 0)}

    def remote(source, dest, sender, receiver, device):
        return pltpu.make_async_remote_copy(
            src_ref=source, dst_ref=dest, send_sem=sender, recv_sem=receiver,
            device_id=device, device_id_type=pl.DeviceIdType.MESH,
        )

    def push(dz, dy, k, device):
        place = spot(dz, dy, k)
        copy = remote(
            pool.at[place], pool.at[place], send_sem.at[len(pending)], recv_sem.at[place], device
        )
        copy.start()
        pending.append(copy)

    up = {"seq": shard(1, 0), "head": head}
    down = {"seq": shard(-1, 0), "head": head}
    across = {"seq": shard(0, 1), "head": head}

    def arrive(dz, dy, k):
        key = (dz % depth, dy % 2, k)
        if key in landed:
            return
        landed.add(key)
        place = spot(dz, dy, k)
        remote(
            pool.at[place], pool.at[place], send_sem.at[0], recv_sem.at[place], across
        ).wait_recv()

    others = list(range(2, classes)) + [1]
    mine = seq * head_count + head
    for k in others:
        copy = remote(
            stage.at[k - 1], pool.at[mine], send_sem.at[len(pending)], recv_sem.at[mine],
            {"seq": seq, "head": lane(k)},
        )
        copy.start()
        pending.append(copy)
    q_copies = []

    def reach(flag):
        if depth % 2:
            return (depth - 1) // 2, (depth - 1) // 2
        return (depth // 2, depth // 2 - 1) if flag else (depth // 2 - 1, depth // 2)

    half = classes // 2
    first_kind, second_kind = range(0, 2), range(2, classes)

    def z_first_own(k):
        arrive(0, 0, k)
        push(0, 0, k, up)
        push(0, 0, k, down)
        push(0, 0, k, across)

    def z_first_hop(k, t):
        plus, minus = reach(k % 2 == 0)
        if t <= plus:
            arrive(-t, 0, k)
            if t < plus:
                push(-t, 0, k, up)
            push(-t, 0, k, across)
        if t <= minus:
            arrive(t, 0, k)
            if t < minus:
                push(t, 0, k, down)
            push(t, 0, k, across)

    def y_first_own(k):
        arrive(0, 0, k)
        push(0, 0, k, across)
        push(0, 0, k, up)
        push(0, 0, k, down)

    def y_first_partner(k):
        arrive(0, 1, k)
        push(0, 1, k, up)
        push(0, 1, k, down)

    def y_first_hop(k, t, dy):
        plus, minus = reach(dy == 0)
        if t <= plus:
            arrive(-t, dy, k)
            if t < plus:
                push(-t, dy, k, up)
        if t <= minus:
            arrive(t, dy, k)
            if t < minus:
                push(t, dy, k, down)

    def fold(dz, dy, kind):
        ks = (0, 1) if kind == 0 else (2, 3)
        for k in ks:
            arrive(dz, dy, k)
        low = (head // 2 + kind) % (head_count // 2) * 2
        place = shard(dz, dy) * head_count + low

        for hd in range(heads_dev):
            cols = slice(hd * HEAD_DIM, (hd + 1) * HEAD_DIM)
            query = q_all[:, :, cols].reshape(tokens, HEAD_DIM)
            old_peak = peak_ref[pl.ds(hd, 1), :]
            new_peak = old_peak
            parts = []
            for n in range(2):
                block = place + n
                gap = query_block - block
                count = jnp.where((gap >= -1) & (gap <= 1), 1, 0)
                for g in range(glob_count):
                    count += jnp.where(glob_ref[g] == block, 1, 0)
                for r in range(rand_count):
                    row = listed[pl.ds(hd * rand_count + r, 1), :]
                    count += jnp.where(row == block, 1, 0)
                count = jnp.where(glob_row > 0, 1, count)
                scores = lax.dot_general(
                    pool[place + n, 0, :, cols], query, (((1,), (1,)), ((), ())),
                    preferred_element_type=jnp.float32,
                ) * (1.0 / math.sqrt(HEAD_DIM))
                top = jnp.max(scores, axis=0, keepdims=True)
                new_peak = jnp.maximum(new_peak, jnp.where(count > 0, top, MASKED))
                parts.append((scores, count))
            fade = jnp.exp(old_peak - new_peak)
            total = total_ref[pl.ds(hd, 1), :] * fade
            acc = acc_ref[hd] * fade
            for n, (scores, count) in enumerate(parts):
                powers = jnp.exp(scores - jnp.where(count > 0, new_peak, -MASKED))
                powers = powers * count.astype(jnp.float32)
                total = total + jnp.sum(powers, axis=0, keepdims=True)
                acc = acc + lax.dot_general(
                    pool[place + n, 1, :, cols], powers.astype(jnp.bfloat16),
                    (((0,), (0,)), ((), ())), preferred_element_type=jnp.float32,
                )
            peak_ref[pl.ds(hd, 1), :] = new_peak
            total_ref[pl.ds(hd, 1), :] = total
            acc_ref[hd] = acc

    z_first_own(0)
    for k in others:
        copy = remote(
            q_stage.at[k - 1], q_all.at[head], q_send_sem.at[k - 1], q_recv_sem.at[head],
            {"seq": seq, "head": lane(k)},
        )
        copy.start()
        q_copies.append(copy)
    z_first_own(1)
    y_first_own(2)
    z_first_hop(0, 1)
    y_first_own(3)
    z_first_hop(1, 1)
    for k in range(1, classes):
        remote(
            q_stage.at[0], q_all.at[lane(k)], q_send_sem.at[0], q_recv_sem.at[lane(k)], across
        ).wait_recv()
    fold(0, 0, 0)
    y_first_partner(2)
    y_first_partner(3)
    fold(0, 0, 1)
    fold(0, 1, 0)
    waiting = [(0, 1, 1)]
    for t in range(1, depth // 2 + 1):
        for k in (2, 3):
            y_first_hop(k, t, 0)
        for k in (0, 1) if t > 1 else ():
            z_first_hop(k, t)
        for item in waiting:
            fold(*item)
        for k in (2, 3):
            y_first_hop(k, t, 1)
        steps = (-t, t) if 2 * t < depth else (t,)
        waiting = [(dz, 0, 0) for dz in steps]
        waiting += [(dz, 0, 1) for dz in steps] + [(dz, 1, 1) for dz in steps]
        waiting += [(dz, 1, 0) for dz in steps]
    for item in waiting:
        fold(*item)
    for hd in range(heads_dev):
        done = acc_ref[hd] / total_ref[pl.ds(hd, 1), :]
        out_ref[:, hd * HEAD_DIM : (hd + 1) * HEAD_DIM] = done.T
    for copy in pending + q_copies:
        copy.wait_send()


def gathered(queries, keys, values, random_blocks, global_blocks):
    seq_count, head_count = lax.axis_size("seq"), lax.axis_size("head")
    rows, width = queries.shape[0], queries.shape[1] // head_count
    heads_dev = width // HEAD_DIM
    tokens = rows * head_count
    rand_count, glob_count = random_blocks.shape[2], global_blocks.shape[0]
    dma = pltpu.SemaphoreType.DMA
    return pl.pallas_call(
        functools.partial(gathered_kernel, seq_count, head_count, rand_count, glob_count),
        out_shape=jax.ShapeDtypeStruct((tokens, width), jnp.float32),
        in_specs=[pl.BlockSpec(memory_space=pl.ANY)] * 3
        + [pl.BlockSpec(memory_space=pltpu.SMEM)] * 2,
        out_specs=pl.BlockSpec(memory_space=pltpu.VMEM),
        scratch_shapes=[
            pltpu.VMEM((seq_count * head_count, 2, rows, width), jnp.bfloat16),
            pltpu.VMEM((head_count, rows, width), jnp.bfloat16),
            pltpu.VMEM((head_count - 1, 2, rows, width), jnp.bfloat16),
            pltpu.VMEM((head_count - 1, rows, width), jnp.bfloat16),
            pltpu.VMEM((heads_dev * rand_count, tokens), jnp.int32),
            pltpu.VMEM((heads_dev, tokens), jnp.float32),
            pltpu.VMEM((heads_dev, tokens), jnp.float32),
            pltpu.VMEM((heads_dev, HEAD_DIM, tokens), jnp.float32),
            dma((3 * head_count,)),
            dma((head_count + 5 * seq_count,)),
            dma((seq_count * head_count,)),
            dma((head_count - 1,)),
            dma((head_count,)),
        ],
        compiler_params=pltpu.CompilerParams(
            collective_id=0, has_side_effects=True, vmem_limit_bytes=40 * 2**20
        ),
    )(queries, keys, values, random_blocks, global_blocks)


def shards(queries, keys, values, random_blocks, global_blocks):
    seq_count, head_count = lax.axis_size("seq"), lax.axis_size("head")
    pool_bytes = 4 * seq_count * queries.size
    fits = pool_bytes <= GATHER_LIMIT and queries.shape[0] == BLK
    if fits and head_count == 4 and seq_count % 2 == 0 and seq_count >= 6:
        return gathered(queries, keys, values, random_blocks, global_blocks)
    return exchanged(queries, keys, values, random_blocks, global_blocks)


def solution(mesh):
    in_specs = (
        P(("seq", "head"), None),
        P(("seq", "head"), None),
        P(("seq", "head"), None),
        P("seq", "head", None),
        P(),
    )
    out_specs = P("seq", "head")
    return jax.shard_map(shards, mesh=mesh, in_specs=in_specs, out_specs=out_specs, check_vma=False)
```

```python
import functools
import math

import jax
import jax.numpy as jnp
from jax import lax
from jax.experimental import pallas as pl
from jax.experimental.pallas import tpu as pltpu
from jax.sharding import PartitionSpec as P

HEAD_DIM = 128
BLK = 64


MASKED = -1e30


def extended(block, sides, width):
    for axis, dim in sides:
        count = lax.axis_size(axis)
        forward = [(i, i + 1) for i in range(count - 1)]
        backward = [(target, source) for source, target in forward]
        low = lax.ppermute(
            lax.slice_in_dim(block, block.shape[dim] - width, None, axis=dim), axis, forward
        )
        high = lax.ppermute(lax.slice_in_dim(block, 0, width, axis=dim), axis, backward)
        block = jnp.concatenate([low, block, high], axis=dim)
    return block


def combined_all(value, axis, join):
    pieces = jax.tree.map(lambda part: lax.all_gather(part, axis), value)
    head = jax.tree.map(lambda part: part[0], pieces)
    tail = jax.tree.map(lambda part: part[1:], pieces)
    so_far, _ = lax.scan(lambda so_far, slab: (join(so_far, slab), None), head, tail)
    return so_far


def merge_parts(former, latter):
    peaks = jnp.maximum(former[0], latter[0])
    former_fade = jnp.exp(former[0] - peaks)
    latter_fade = jnp.exp(latter[0] - peaks)
    return (
        peaks,
        former[1] * former_fade + latter[1] * latter_fade,
        former[2] * former_fade[..., None] + latter[2] * latter_fade[..., None],
    )


def soft_parts(scores):
    peaks = jnp.max(scores, axis=(-2, -1))
    powers = jnp.exp(scores - peaks[..., None, None])
    return (peaks, jnp.sum(powers, axis=(-2, -1)), powers.astype(jnp.bfloat16))


def make_requests(rand_lists, seq_count, capacity):
    blk_dev, heads_dev, rand_count = rand_lists.shape
    flat_list = rand_lists.reshape(-1)
    owners = flat_list // blk_dev
    head_ids = jnp.broadcast_to(
        jnp.arange(heads_dev, dtype=jnp.int32)[None, :, None], rand_lists.shape
    ).reshape(-1)
    item_ids = flat_list % blk_dev * heads_dev + head_ids
    position = jnp.arange(flat_list.shape[0], dtype=jnp.int32)
    earlier = (owners[:, None] == owners[None, :]) & (position[None, :] < position[:, None])
    slot_ids = owners * capacity + jnp.sum(earlier.astype(jnp.int32), axis=1)
    requests = jnp.zeros((seq_count * capacity,), jnp.int32).at[slot_ids].set(item_ids)
    sources = jnp.zeros((seq_count * capacity,), jnp.int32).at[slot_ids].set(position)
    return (requests.reshape(seq_count, capacity), slot_ids, sources)


def exchanged(queries, keys, values, random_blocks, global_blocks):
    seq_count = lax.axis_size("seq")
    seq_index = lax.axis_index("seq")
    query_rows, key_rows, value_rows = (
        lax.all_to_all(queries, "head", split_axis=1, concat_axis=0, tiled=True),
        lax.all_to_all(keys, "head", split_axis=1, concat_axis=0, tiled=True),
        lax.all_to_all(values, "head", split_axis=1, concat_axis=0, tiled=True),
    )
    tokens = query_rows.shape[0]
    blk_dev = tokens // BLK
    heads_dev = query_rows.shape[1] // HEAD_DIM
    rand_count = random_blocks.shape[2]
    glob_count = global_blocks.shape[0]
    total_blocks = blk_dev * seq_count
    first_block = seq_index * blk_dev
    capacity = (blk_dev * heads_dev * rand_count * 3 // 2 + seq_count - 1) // seq_count
    score_scale = 1.0 / math.sqrt(HEAD_DIM)
    shape_four = (blk_dev, BLK, heads_dev, HEAD_DIM)
    query_four = query_rows.reshape(shape_four)
    key_four = key_rows.reshape(shape_four)
    value_four = value_rows.reshape(shape_four)
    paired = jnp.stack([key_rows, value_rows])
    padded = extended(paired, (("seq", 1),), BLK)
    padded = padded.reshape(2, blk_dev + 2, BLK, heads_dev, HEAD_DIM)
    window = jnp.stack([padded[:, offset : offset + blk_dev] for offset in range(3)], axis=2)
    near_ids = (
        first_block
        + jnp.arange(blk_dev, dtype=jnp.int32)[:, None]
        + jnp.arange(-1, 2, dtype=jnp.int32)[None, :]
    )
    inside = (near_ids >= 0) & (near_ids < total_blocks)
    stacked = jnp.stack([query_rows, key_rows, value_rows]).reshape(
        3, blk_dev, BLK, heads_dev * HEAD_DIM
    )
    owned_mask = global_blocks // blk_dev == seq_index
    local_ids = jnp.where(owned_mask, global_blocks - first_block, 0)
    picked = (
        jnp.take(stacked, local_ids, axis=1).astype(jnp.float32)
        * owned_mask.astype(jnp.float32)[None, :, None, None]
    )
    glob_rows = lax.psum(picked, "seq").astype(jnp.bfloat16)
    glob_rows = glob_rows.reshape(3, glob_count, BLK, heads_dev, HEAD_DIM)
    requests, slot_ids, sources = make_requests(random_blocks, seq_count, capacity)
    incoming = lax.all_to_all(requests, "seq", split_axis=0, concat_axis=0, tiled=True)

    def by_block(row_data):
        return (
            row_data.reshape(shape_four)
            .transpose(0, 2, 1, 3)
            .reshape(blk_dev * heads_dev, BLK, HEAD_DIM)
        )

    pair_blocks = jnp.stack([by_block(key_rows), by_block(value_rows)], axis=1)
    served = pair_blocks[incoming]
    key_win, value_win = (window[0], window[1])
    win_scores = (
        jnp.einsum("jqhd,jwkhd->jhqwk", query_four, key_win, preferred_element_type=jnp.float32)
        * score_scale
    )
    win_scores = jnp.where(inside[:, None, None, :, None], win_scores, MASKED)
    glob_scores = (
        jnp.einsum("jqhd,gkhd->jhqgk", query_four, glob_rows[1], preferred_element_type=jnp.float32)
        * score_scale
    )
    split_at = 3 + glob_count
    arrived_pairs = lax.all_to_all(served, "seq", split_axis=0, concat_axis=0, tiled=True)
    tail = arrived_pairs.shape[2:]
    rand_pairs = arrived_pairs.reshape((seq_count * capacity,) + tail)[slot_ids].reshape(
        (blk_dev, heads_dev, rand_count) + tail
    )
    rand_scores = (
        jnp.einsum(
            "jqhd,jhrkd->jhqrk",
            query_four,
            rand_pairs[:, :, :, 0],
            preferred_element_type=jnp.float32,
        )
        * score_scale
    )
    peaks, totals, weights = soft_parts(
        jnp.concatenate([win_scores, glob_scores, rand_scores], axis=3)
    )
    sums_all = jnp.einsum(
        "jhqwk,jwkhd->jhqd", weights[:, :, :, 0:3], value_win, preferred_element_type=jnp.float32
    )
    sums_all = sums_all + jnp.einsum(
        "jhqgk,gkhd->jhqd",
        weights[:, :, :, 3:split_at],
        glob_rows[2],
        preferred_element_type=jnp.float32,
    )
    sums_all = sums_all + jnp.einsum(
        "jhqrk,jhrkd->jhqd",
        weights[:, :, :, split_at:],
        rand_pairs[:, :, :, 1],
        preferred_element_type=jnp.float32,
    )
    running = (peaks, totals, sums_all)
    sparse_out = (running[2] / running[1][..., None]).transpose(0, 2, 1, 3)
    full_scores = (
        jnp.einsum("gqhd,jkhd->hgqjk", glob_rows[0], key_four, preferred_element_type=jnp.float32)
        * score_scale
    )
    full_peaks, full_totals, full_weights = soft_parts(full_scores)
    full_sum = jnp.einsum(
        "hgqjk,jkhd->hgqd", full_weights, value_four, preferred_element_type=jnp.float32
    )
    merged = combined_all((full_peaks, full_totals, full_sum), "seq", merge_parts)
    glob_out = (merged[2] / merged[1][..., None]).transpose(1, 2, 0, 3)
    block_ids = first_block + jnp.arange(blk_dev, dtype=jnp.int32)
    result = sparse_out
    for glob_id in range(glob_count):
        matches = (block_ids == global_blocks[glob_id])[:, None, None, None]
        result = jnp.where(matches, glob_out[glob_id][None], result)
    return result.reshape(tokens, heads_dev * HEAD_DIM)


GATHER_LIMIT = 16 * 2**20


def gathered_kernel(
    seq_count, head_count, rand_count, glob_count,
    q_hbm, k_hbm, v_hbm, rand_ref, glob_ref, out_ref,
    pool, rand_vmem, q_all, stage, q_stage, listed, peak_ref, total_ref, acc_ref,
    local_sem, send_sem, recv_sem, q_recv_sem,
):
    seq = lax.axis_index("seq")
    head = lax.axis_index("head")
    depth = seq_count // 2
    z, y = seq // 2, seq % 2
    rows, width = q_all.shape[1], q_all.shape[2]
    heads_dev = width // HEAD_DIM
    tokens = head_count * rows
    classes = head_count

    def lane(k):
        return ((head // 2 + k // 2) % (head_count // 2)) * 2 + (head % 2 + k % 2) % 2

    def shard(dz, dy):
        return ((z + dz) % depth) * 2 + (y + dy) % 2

    def spot(dz, dy, k):
        return shard(dz, dy) * head_count + lane(k)

    names_copy = pltpu.make_async_copy(rand_ref, rand_vmem, local_sem.at[3 * classes])
    names_copy.start()
    loads = []
    for k in range(classes):
        cols = pl.ds(pl.multiple_of(lane(k) * width, 128), width)
        target = pool.at[spot(0, 0, 0)] if k == 0 else stage.at[k - 1]
        q_target = q_all.at[head] if k == 0 else q_stage.at[k - 1]
        trio = []
        for n, (source, dest) in enumerate(
            ((k_hbm, target.at[0]), (v_hbm, target.at[1]), (q_hbm, q_target))
        ):
            trio.append(pltpu.make_async_copy(source.at[:, cols], dest, local_sem.at[k * 3 + n]))
        loads.append(trio)
    for trio in loads:
        trio[0].start()
        trio[1].start()
    for trio in loads:
        trio[2].start()

    barrier = pltpu.get_barrier_semaphore()
    friends = [{"seq": seq, "head": lane(k)} for k in range(1, classes)]
    friends.append({"seq": shard(0, 1), "head": head})
    up = {"seq": shard(1, 0), "head": head}
    down = {"seq": shard(-1, 0), "head": head}
    across = {"seq": shard(0, 1), "head": head}

    def greet(friend):
        pl.semaphore_signal(barrier, inc=1, device_id=friend, device_id_type=pl.DeviceIdType.MESH)

    for friend in friends:
        greet(friend)
    pl.when(z < depth - 1)(lambda: greet(up))
    pl.when(z > 0)(lambda: greet(down))
    names_copy.wait()

    query_block = seq * (tokens // BLK) + lax.broadcasted_iota(jnp.int32, (1, tokens), 1) // BLK
    local_block = lax.broadcasted_iota(jnp.int32, (1, tokens), 1) // BLK
    for hd in range(heads_dev):
        for r in range(rand_count):
            names = jnp.zeros((1, tokens), jnp.int32)
            for b in range(tokens // BLK):
                names = jnp.where(local_block == b, rand_vmem[b, pl.ds(hd, 1), pl.ds(r, 1)], names)
            listed[pl.ds(hd * rand_count + r, 1), :] = names
    is_glob = query_block == glob_ref[0]
    for g in range(1, glob_count):
        is_glob = is_glob | (query_block == glob_ref[g])
    glob_row = jnp.where(is_glob, 1, 0)
    peak_ref[...] = jnp.full_like(peak_ref, MASKED)
    total_ref[...] = jnp.zeros_like(total_ref)
    acc_ref[...] = jnp.zeros_like(acc_ref)

    for trio in loads:
        trio[0].wait()
        trio[1].wait()
    for trio in loads:
        trio[2].wait()
    line_friends = (z + depth - 1) // depth + (2 * depth - 2 - z) // depth
    pl.semaphore_wait(barrier, len(friends) + line_friends)

    pending = []
    landed = {(0, 0, 0, 2)}
    everywhere = z >= 0
    cuts = [(2,)] * (classes - 1) + [(0, 1)]
    y_first = {(classes - 1, 0)}

    def remote(source, dest, sender, receiver, device):
        return pltpu.make_async_remote_copy(
            src_ref=source, dst_ref=dest, send_sem=sender, recv_sem=receiver,
            device_id=device, device_id_type=pl.DeviceIdType.MESH,
        )

    def view(ref, place, cut):
        return ref.at[place] if cut == 2 else ref.at[place, cut]

    def post(source, dest, receiver, device, when=everywhere):
        sender = send_sem.at[len(pending)]
        pl.when(when)(lambda: remote(source, dest, sender, receiver, device).start())
        pending.append((source, dest, sender, receiver, device, when))

    def push(dz, dy, k, cut, device, when=everywhere):
        place = spot(dz, dy, k)
        piece = view(pool, place, cut)
        post(piece, piece, recv_sem.at[place, cut % 2], device, when)

    def exists(dz):
        return z >= -dz if dz < 0 else z + dz < depth

    def arrive(dz, dy, k, cut, when=everywhere):
        key = (dz, dy, k, cut)
        if key in landed:
            return
        landed.add(key)
        place = spot(dz, dy, k)
        piece = view(pool, place, cut)
        pl.when(when)(
            lambda: remote(
                piece, piece, send_sem.at[0], recv_sem.at[place, cut % 2], across
            ).wait_recv()
        )

    others = list(range(2, classes)) + [1]
    mine = seq * head_count + head
    for k in others:
        for cut in cuts[k]:
            post(
                view(stage, k - 1, cut), view(pool, mine, cut), recv_sem.at[mine, cut % 2],
                {"seq": seq, "head": lane(k)},
            )

    def own(k):
        for cut in cuts[k]:
            arrive(0, 0, k, cut)
            push(0, 0, k, cut, across)
            push(0, 0, k, cut, up, z < depth - 1)
            push(0, 0, k, cut, down, z > 0)

    def onward(dz, dy, k, cut, cross):
        here = exists(dz)
        arrive(dz, dy, k, cut, here)
        if dz < 0 and -dz < depth - 1:
            push(dz, dy, k, cut, up, here & (z < depth - 1))
        if dz > 0 and dz < depth - 1:
            push(dz, dy, k, cut, down, here & (z > 0))
        if cross:
            push(dz, dy, k, cut, across, here)

    def hop(k, t):
        for cut in cuts[k]:
            early = (k, cut) in y_first
            for dz in (-t, t):
                onward(dz, 0, k, cut, not early)

    def partner_hop(t):
        for k, cut in sorted(y_first):
            for dz in (-t, t):
                onward(dz, 1, k, cut, False)

    def partner():
        for k, cut in sorted(y_first):
            arrive(0, 1, k, cut)
            push(0, 1, k, cut, up, z < depth - 1)
            push(0, 1, k, cut, down, z > 0)

    def fold(dz, dy, kind):
        ks = (0, 1) if kind == 0 else (2, 3)
        here = exists(dz)
        for k in ks:
            for cut in cuts[k]:
                arrive(dz, dy, k, cut, here)
        pl.when(here)(functools.partial(folded, dz, dy, kind))

    def folded(dz, dy, kind):
        low = (head // 2 + kind) % (head_count // 2) * 2
        place = shard(dz, dy) * head_count + low

        for hd in range(heads_dev):
            cols = slice(hd * HEAD_DIM, (hd + 1) * HEAD_DIM)
            query = q_all[:, :, cols].reshape(tokens, HEAD_DIM)
            old_peak = peak_ref[pl.ds(hd, 1), :]
            new_peak = old_peak
            parts = []
            for n in range(2):
                block = place + n
                gap = query_block - block
                count = jnp.where((gap >= -1) & (gap <= 1), 1, 0)
                for g in range(glob_count):
                    count += jnp.where(glob_ref[g] == block, 1, 0)
                for r in range(rand_count):
                    row = listed[pl.ds(hd * rand_count + r, 1), :]
                    count += jnp.where(row == block, 1, 0)
                count = jnp.where(glob_row > 0, 1, count)
                scores = lax.dot_general(
                    pool[place + n, 0, :, cols], query, (((1,), (1,)), ((), ())),
                    preferred_element_type=jnp.float32,
                ) * (1.0 / math.sqrt(HEAD_DIM))
                top = jnp.max(scores, axis=0, keepdims=True)
                new_peak = jnp.maximum(new_peak, jnp.where(count > 0, top, MASKED))
                parts.append((scores, count))
            fade = jnp.exp(old_peak - new_peak)
            total = total_ref[pl.ds(hd, 1), :] * fade
            acc = acc_ref[hd] * fade
            for n, (scores, count) in enumerate(parts):
                powers = jnp.exp(scores - jnp.where(count > 0, new_peak, -MASKED))
                powers = powers * count.astype(jnp.float32)
                total = total + jnp.sum(powers, axis=0, keepdims=True)
                acc = acc + lax.dot_general(
                    pool[place + n, 1, :, cols], powers.astype(jnp.bfloat16),
                    (((0,), (0,)), ((), ())), preferred_element_type=jnp.float32,
                )
            peak_ref[pl.ds(hd, 1), :] = new_peak
            total_ref[pl.ds(hd, 1), :] = total
            acc_ref[hd] = acc

    own(0)
    for k in others:
        post(q_stage.at[k - 1], q_all.at[head], q_recv_sem.at[head], {"seq": seq, "head": lane(k)})
    own(1)
    own(2)
    hop(0, 1)
    own(3)
    hop(1, 1)
    partner()
    for k in range(1, classes):
        remote(
            q_stage.at[0], q_all.at[lane(k)], send_sem.at[0], q_recv_sem.at[lane(k)], across
        ).wait_recv()
    fold(0, 0, 0)
    hop(2, 1)
    fold(0, 0, 1)
    hop(3, 1)
    fold(0, 1, 0)
    partner_hop(1)
    waiting = [(0, 1, 1)]
    for t in range(1, depth):
        waiting += [(dz, dy, kind) for dy in (0, 1) for kind in (0, 1) for dz in (-t, t)]
        if t + 1 < depth:
            for k in range(classes):
                hop(k, t + 1)
                for item in waiting[:2]:
                    fold(*item)
                waiting = waiting[2:]
            partner_hop(t + 1)
    for item in waiting:
        fold(*item)
    for hd in range(heads_dev):
        done = acc_ref[hd] / total_ref[pl.ds(hd, 1), :]
        out_ref[:, hd * HEAD_DIM : (hd + 1) * HEAD_DIM] = done.T
    for *parts, when in pending:
        pl.when(when)(lambda parts=parts: remote(*parts).wait_send())


def gathered(queries, keys, values, random_blocks, global_blocks):
    seq_count, head_count = lax.axis_size("seq"), lax.axis_size("head")
    rows, width = queries.shape[0], queries.shape[1] // head_count
    heads_dev = width // HEAD_DIM
    tokens = rows * head_count
    rand_count, glob_count = random_blocks.shape[2], global_blocks.shape[0]
    dma = pltpu.SemaphoreType.DMA
    return pl.pallas_call(
        functools.partial(gathered_kernel, seq_count, head_count, rand_count, glob_count),
        out_shape=jax.ShapeDtypeStruct((tokens, width), jnp.float32),
        in_specs=[pl.BlockSpec(memory_space=pltpu.HBM)] * 4
        + [pl.BlockSpec(memory_space=pltpu.SMEM)],
        out_specs=pl.BlockSpec(memory_space=pltpu.VMEM),
        scratch_shapes=[
            pltpu.VMEM((seq_count * head_count, 2, rows, width), jnp.bfloat16),
            pltpu.VMEM(random_blocks.shape, jnp.int32),
            pltpu.VMEM((head_count, rows, width), jnp.bfloat16),
            pltpu.VMEM((head_count - 1, 2, rows, width), jnp.bfloat16),
            pltpu.VMEM((head_count - 1, rows, width), jnp.bfloat16),
            pltpu.VMEM((heads_dev * rand_count, tokens), jnp.int32),
            pltpu.VMEM((heads_dev, tokens), jnp.float32),
            pltpu.VMEM((heads_dev, tokens), jnp.float32),
            pltpu.VMEM((heads_dev, HEAD_DIM, tokens), jnp.float32),
            dma((3 * head_count + 1,)),
            dma((10 * seq_count + 24,)),
            dma((seq_count * head_count, 2)),
            dma((head_count,)),
        ],
        compiler_params=pltpu.CompilerParams(
            collective_id=0, has_side_effects=True, vmem_limit_bytes=40 * 2**20
        ),
    )(queries, keys, values, random_blocks, global_blocks)


def shards(queries, keys, values, random_blocks, global_blocks):
    seq_count, head_count = lax.axis_size("seq"), lax.axis_size("head")
    pool_bytes = 4 * seq_count * queries.size
    fits = pool_bytes <= GATHER_LIMIT and queries.shape[0] == BLK
    if fits and head_count == 4 and seq_count % 2 == 0 and seq_count >= 6:
        return gathered(queries, keys, values, random_blocks, global_blocks)
    return exchanged(queries, keys, values, random_blocks, global_blocks)


def solution(mesh):
    in_specs = (
        P(("seq", "head"), None),
        P(("seq", "head"), None),
        P(("seq", "head"), None),
        P("seq", "head", None),
        P(),
    )
    out_specs = P("seq", "head")
    return jax.shard_map(shards, mesh=mesh, in_specs=in_specs, out_specs=out_specs, check_vma=False)
```

```python
import functools
import math

import jax
import jax.numpy as jnp
from jax import lax
from jax.experimental import pallas as pl
from jax.experimental.pallas import tpu as pltpu
from jax.sharding import PartitionSpec as P

HEAD_DIM = 128
BLK = 64


MASKED = -1e30


def extended(block, sides, width):
    for axis, dim in sides:
        count = lax.axis_size(axis)
        forward = [(i, i + 1) for i in range(count - 1)]
        backward = [(target, source) for source, target in forward]
        low = lax.ppermute(
            lax.slice_in_dim(block, block.shape[dim] - width, None, axis=dim), axis, forward
        )
        high = lax.ppermute(lax.slice_in_dim(block, 0, width, axis=dim), axis, backward)
        block = jnp.concatenate([low, block, high], axis=dim)
    return block


def combined_all(value, axis, join):
    pieces = jax.tree.map(lambda part: lax.all_gather(part, axis), value)
    head = jax.tree.map(lambda part: part[0], pieces)
    tail = jax.tree.map(lambda part: part[1:], pieces)
    so_far, _ = lax.scan(lambda so_far, slab: (join(so_far, slab), None), head, tail)
    return so_far


def merge_parts(former, latter):
    peaks = jnp.maximum(former[0], latter[0])
    former_fade = jnp.exp(former[0] - peaks)
    latter_fade = jnp.exp(latter[0] - peaks)
    return (
        peaks,
        former[1] * former_fade + latter[1] * latter_fade,
        former[2] * former_fade[..., None] + latter[2] * latter_fade[..., None],
    )


def soft_parts(scores):
    peaks = jnp.max(scores, axis=(-2, -1))
    powers = jnp.exp(scores - peaks[..., None, None])
    return (peaks, jnp.sum(powers, axis=(-2, -1)), powers.astype(jnp.bfloat16))


def make_requests(rand_lists, seq_count, capacity):
    blk_dev, heads_dev, rand_count = rand_lists.shape
    flat_list = rand_lists.reshape(-1)
    owners = flat_list // blk_dev
    head_ids = jnp.broadcast_to(
        jnp.arange(heads_dev, dtype=jnp.int32)[None, :, None], rand_lists.shape
    ).reshape(-1)
    item_ids = flat_list % blk_dev * heads_dev + head_ids
    position = jnp.arange(flat_list.shape[0], dtype=jnp.int32)
    earlier = (owners[:, None] == owners[None, :]) & (position[None, :] < position[:, None])
    slot_ids = owners * capacity + jnp.sum(earlier.astype(jnp.int32), axis=1)
    requests = jnp.zeros((seq_count * capacity,), jnp.int32).at[slot_ids].set(item_ids)
    sources = jnp.zeros((seq_count * capacity,), jnp.int32).at[slot_ids].set(position)
    return (requests.reshape(seq_count, capacity), slot_ids, sources)


def exchanged(queries, keys, values, random_blocks, global_blocks):
    seq_count = lax.axis_size("seq")
    seq_index = lax.axis_index("seq")
    query_rows, key_rows, value_rows = (
        lax.all_to_all(queries, "head", split_axis=1, concat_axis=0, tiled=True),
        lax.all_to_all(keys, "head", split_axis=1, concat_axis=0, tiled=True),
        lax.all_to_all(values, "head", split_axis=1, concat_axis=0, tiled=True),
    )
    tokens = query_rows.shape[0]
    blk_dev = tokens // BLK
    heads_dev = query_rows.shape[1] // HEAD_DIM
    rand_count = random_blocks.shape[2]
    glob_count = global_blocks.shape[0]
    total_blocks = blk_dev * seq_count
    first_block = seq_index * blk_dev
    capacity = (blk_dev * heads_dev * rand_count * 3 // 2 + seq_count - 1) // seq_count
    score_scale = 1.0 / math.sqrt(HEAD_DIM)
    shape_four = (blk_dev, BLK, heads_dev, HEAD_DIM)
    query_four = query_rows.reshape(shape_four)
    key_four = key_rows.reshape(shape_four)
    value_four = value_rows.reshape(shape_four)
    paired = jnp.stack([key_rows, value_rows])
    padded = extended(paired, (("seq", 1),), BLK)
    padded = padded.reshape(2, blk_dev + 2, BLK, heads_dev, HEAD_DIM)
    window = jnp.stack([padded[:, offset : offset + blk_dev] for offset in range(3)], axis=2)
    near_ids = (
        first_block
        + jnp.arange(blk_dev, dtype=jnp.int32)[:, None]
        + jnp.arange(-1, 2, dtype=jnp.int32)[None, :]
    )
    inside = (near_ids >= 0) & (near_ids < total_blocks)
    stacked = jnp.stack([query_rows, key_rows, value_rows]).reshape(
        3, blk_dev, BLK, heads_dev * HEAD_DIM
    )
    owned_mask = global_blocks // blk_dev == seq_index
    local_ids = jnp.where(owned_mask, global_blocks - first_block, 0)
    picked = (
        jnp.take(stacked, local_ids, axis=1).astype(jnp.float32)
        * owned_mask.astype(jnp.float32)[None, :, None, None]
    )
    glob_rows = lax.psum(picked, "seq").astype(jnp.bfloat16)
    glob_rows = glob_rows.reshape(3, glob_count, BLK, heads_dev, HEAD_DIM)
    requests, slot_ids, sources = make_requests(random_blocks, seq_count, capacity)
    incoming = lax.all_to_all(requests, "seq", split_axis=0, concat_axis=0, tiled=True)

    def by_block(row_data):
        return (
            row_data.reshape(shape_four)
            .transpose(0, 2, 1, 3)
            .reshape(blk_dev * heads_dev, BLK, HEAD_DIM)
        )

    pair_blocks = jnp.stack([by_block(key_rows), by_block(value_rows)], axis=1)
    served = pair_blocks[incoming]
    key_win, value_win = (window[0], window[1])
    win_scores = (
        jnp.einsum("jqhd,jwkhd->jhqwk", query_four, key_win, preferred_element_type=jnp.float32)
        * score_scale
    )
    win_scores = jnp.where(inside[:, None, None, :, None], win_scores, MASKED)
    glob_scores = (
        jnp.einsum("jqhd,gkhd->jhqgk", query_four, glob_rows[1], preferred_element_type=jnp.float32)
        * score_scale
    )
    split_at = 3 + glob_count
    arrived_pairs = lax.all_to_all(served, "seq", split_axis=0, concat_axis=0, tiled=True)
    tail = arrived_pairs.shape[2:]
    rand_pairs = arrived_pairs.reshape((seq_count * capacity,) + tail)[slot_ids].reshape(
        (blk_dev, heads_dev, rand_count) + tail
    )
    rand_scores = (
        jnp.einsum(
            "jqhd,jhrkd->jhqrk",
            query_four,
            rand_pairs[:, :, :, 0],
            preferred_element_type=jnp.float32,
        )
        * score_scale
    )
    peaks, totals, weights = soft_parts(
        jnp.concatenate([win_scores, glob_scores, rand_scores], axis=3)
    )
    sums_all = jnp.einsum(
        "jhqwk,jwkhd->jhqd", weights[:, :, :, 0:3], value_win, preferred_element_type=jnp.float32
    )
    sums_all = sums_all + jnp.einsum(
        "jhqgk,gkhd->jhqd",
        weights[:, :, :, 3:split_at],
        glob_rows[2],
        preferred_element_type=jnp.float32,
    )
    sums_all = sums_all + jnp.einsum(
        "jhqrk,jhrkd->jhqd",
        weights[:, :, :, split_at:],
        rand_pairs[:, :, :, 1],
        preferred_element_type=jnp.float32,
    )
    running = (peaks, totals, sums_all)
    sparse_out = (running[2] / running[1][..., None]).transpose(0, 2, 1, 3)
    full_scores = (
        jnp.einsum("gqhd,jkhd->hgqjk", glob_rows[0], key_four, preferred_element_type=jnp.float32)
        * score_scale
    )
    full_peaks, full_totals, full_weights = soft_parts(full_scores)
    full_sum = jnp.einsum(
        "hgqjk,jkhd->hgqd", full_weights, value_four, preferred_element_type=jnp.float32
    )
    merged = combined_all((full_peaks, full_totals, full_sum), "seq", merge_parts)
    glob_out = (merged[2] / merged[1][..., None]).transpose(1, 2, 0, 3)
    block_ids = first_block + jnp.arange(blk_dev, dtype=jnp.int32)
    result = sparse_out
    for glob_id in range(glob_count):
        matches = (block_ids == global_blocks[glob_id])[:, None, None, None]
        result = jnp.where(matches, glob_out[glob_id][None], result)
    return result.reshape(tokens, heads_dev * HEAD_DIM)


GATHER_LIMIT = 16 * 2**20


def gathered_kernel(
    seq_count, head_count, rand_count, glob_count,
    q_hbm, k_hbm, v_hbm, rand_ref, glob_ref, out_ref,
    pool, rand_vmem, q_all, stage, q_stage, listed, peak_ref, total_ref, acc_ref,
    local_sem, send_sem, recv_sem, q_recv_sem,
):
    seq = lax.axis_index("seq")
    head = lax.axis_index("head")
    depth = seq_count // 2
    z, y = seq // 2, seq % 2
    rows, width = q_all.shape[1], q_all.shape[2]
    heads_dev = width // HEAD_DIM
    tokens = head_count * rows
    classes = head_count

    def lane(k):
        return ((head // 2 + k // 2) % (head_count // 2)) * 2 + (head % 2 + k % 2) % 2

    def shard(dz, dy):
        return ((z + dz) % depth) * 2 + (y + dy) % 2

    def spot(dz, dy, k):
        return shard(dz, dy) * head_count + lane(k)

    names_copy = pltpu.make_async_copy(rand_ref, rand_vmem, local_sem.at[3 * classes])
    names_copy.start()
    loads = []
    for k in range(classes):
        cols = pl.ds(pl.multiple_of(lane(k) * width, 128), width)
        target = pool.at[spot(0, 0, 0)] if k == 0 else stage.at[k - 1]
        q_target = q_all.at[head] if k == 0 else q_stage.at[k - 1]
        trio = []
        for n, (source, dest) in enumerate(
            ((k_hbm, target.at[0]), (v_hbm, target.at[1]), (q_hbm, q_target))
        ):
            trio.append(pltpu.make_async_copy(source.at[:, cols], dest, local_sem.at[k * 3 + n]))
        loads.append(trio)
    for trio in loads:
        trio[0].start()
        trio[1].start()
    for trio in loads:
        trio[2].start()

    barrier = pltpu.get_barrier_semaphore()
    friends = [{"seq": seq, "head": lane(k)} for k in range(1, classes)]
    friends.append({"seq": shard(0, 1), "head": head})
    up = {"seq": shard(1, 0), "head": head}
    down = {"seq": shard(-1, 0), "head": head}
    across = {"seq": shard(0, 1), "head": head}

    def greet(friend):
        pl.semaphore_signal(barrier, inc=1, device_id=friend, device_id_type=pl.DeviceIdType.MESH)

    for friend in friends:
        greet(friend)
    pl.when(z < depth - 1)(lambda: greet(up))
    pl.when(z > 0)(lambda: greet(down))
    names_copy.wait()

    query_block = seq * (tokens // BLK) + lax.broadcasted_iota(jnp.int32, (1, tokens), 1) // BLK
    local_block = lax.broadcasted_iota(jnp.int32, (1, tokens), 1) // BLK
    for hd in range(heads_dev):
        for r in range(rand_count):
            names = jnp.zeros((1, tokens), jnp.int32)
            for b in range(tokens // BLK):
                names = jnp.where(local_block == b, rand_vmem[b, pl.ds(hd, 1), pl.ds(r, 1)], names)
            listed[pl.ds(hd * rand_count + r, 1), :] = names
    is_glob = query_block == glob_ref[0]
    for g in range(1, glob_count):
        is_glob = is_glob | (query_block == glob_ref[g])
    glob_row = jnp.where(is_glob, 1, 0)
    peak_ref[...] = jnp.full_like(peak_ref, MASKED)
    total_ref[...] = jnp.zeros_like(total_ref)
    acc_ref[...] = jnp.zeros_like(acc_ref)

    for trio in loads:
        trio[0].wait()
        trio[1].wait()
    for trio in loads:
        trio[2].wait()
    line_friends = (z + depth - 1) // depth + (2 * depth - 2 - z) // depth
    pl.semaphore_wait(barrier, len(friends) + line_friends)

    pending = []
    landed = {(0, 0, 0, 2)}
    everywhere = z >= 0
    cuts = [(2,)] * (classes - 1) + [(0, 1)]
    y_first = {(classes - 1, 0)}

    def remote(source, dest, sender, receiver, device):
        return pltpu.make_async_remote_copy(
            src_ref=source, dst_ref=dest, send_sem=sender, recv_sem=receiver,
            device_id=device, device_id_type=pl.DeviceIdType.MESH,
        )

    def view(ref, place, cut):
        return ref.at[place] if cut == 2 else ref.at[place, cut]

    def post(source, dest, receiver, device, when=everywhere):
        sender = send_sem.at[len(pending)]
        pl.when(when)(lambda: remote(source, dest, sender, receiver, device).start())
        pending.append((source, dest, sender, receiver, device, when))

    def push(dz, dy, k, cut, device, when=everywhere):
        place = spot(dz, dy, k)
        piece = view(pool, place, cut)
        post(piece, piece, recv_sem.at[place, cut % 2], device, when)

    def exists(dz):
        return z >= -dz if dz < 0 else z + dz < depth

    def arrive(dz, dy, k, cut, when=everywhere):
        key = (dz, dy, k, cut)
        if key in landed:
            return
        landed.add(key)
        place = spot(dz, dy, k)
        piece = view(pool, place, cut)
        pl.when(when)(
            lambda: remote(
                piece, piece, send_sem.at[0], recv_sem.at[place, cut % 2], across
            ).wait_recv()
        )

    others = list(range(2, classes)) + [1]
    mine = seq * head_count + head
    for k in others:
        for cut in cuts[k]:
            post(
                view(stage, k - 1, cut), view(pool, mine, cut), recv_sem.at[mine, cut % 2],
                {"seq": seq, "head": lane(k)},
            )

    def own(k):
        for cut in cuts[k]:
            arrive(0, 0, k, cut)
            push(0, 0, k, cut, across)
            push(0, 0, k, cut, up, z < depth - 1)
            push(0, 0, k, cut, down, z > 0)

    def onward(dz, dy, k, cut, cross):
        here = exists(dz)
        arrive(dz, dy, k, cut, here)
        if dz < 0 and -dz < depth - 1:
            push(dz, dy, k, cut, up, here & (z < depth - 1))
        if dz > 0 and dz < depth - 1:
            push(dz, dy, k, cut, down, here & (z > 0))
        if cross:
            push(dz, dy, k, cut, across, here)

    def hop(k, t):
        for cut in cuts[k]:
            early = (k, cut) in y_first
            for dz in (-t, t):
                onward(dz, 0, k, cut, not early)

    def partner_hop(t):
        for k, cut in sorted(y_first):
            for dz in (-t, t):
                onward(dz, 1, k, cut, False)

    def partner():
        for k, cut in sorted(y_first):
            arrive(0, 1, k, cut)
            push(0, 1, k, cut, up, z < depth - 1)
            push(0, 1, k, cut, down, z > 0)

    def fold(dz, dy, kind):
        ks = (0, 1) if kind == 0 else (2, 3)
        here = exists(dz)
        for k in ks:
            for cut in cuts[k]:
                arrive(dz, dy, k, cut, here)
        pl.when(here)(functools.partial(folded, dz, dy, kind))

    def folded(dz, dy, kind):
        low = (head // 2 + kind) % (head_count // 2) * 2
        place = shard(dz, dy) * head_count + low

        for hd in range(heads_dev):
            cols = slice(hd * HEAD_DIM, (hd + 1) * HEAD_DIM)
            query = q_all[:, :, cols].reshape(tokens, HEAD_DIM)
            old_peak = peak_ref[pl.ds(hd, 1), :]
            new_peak = old_peak
            parts = []
            for n in range(2):
                block = place + n
                gap = query_block - block
                count = jnp.where((gap >= -1) & (gap <= 1), 1, 0)
                for g in range(glob_count):
                    count += jnp.where(glob_ref[g] == block, 1, 0)
                for r in range(rand_count):
                    row = listed[pl.ds(hd * rand_count + r, 1), :]
                    count += jnp.where(row == block, 1, 0)
                count = jnp.where(glob_row > 0, 1, count)
                scores = lax.dot_general(
                    pool[place + n, 0, :, cols], query, (((1,), (1,)), ((), ())),
                    preferred_element_type=jnp.float32,
                ) * (1.0 / math.sqrt(HEAD_DIM))
                top = jnp.max(scores, axis=0, keepdims=True)
                new_peak = jnp.maximum(new_peak, jnp.where(count > 0, top, MASKED))
                parts.append((scores, count))
            fade = jnp.exp(old_peak - new_peak)
            total = total_ref[pl.ds(hd, 1), :] * fade
            acc = acc_ref[hd] * fade
            for n, (scores, count) in enumerate(parts):
                powers = jnp.exp(scores - jnp.where(count > 0, new_peak, -MASKED))
                powers = powers * count.astype(jnp.float32)
                total = total + jnp.sum(powers, axis=0, keepdims=True)
                acc = acc + lax.dot_general(
                    pool[place + n, 1, :, cols], powers.astype(jnp.bfloat16),
                    (((0,), (0,)), ((), ())), preferred_element_type=jnp.float32,
                )
            peak_ref[pl.ds(hd, 1), :] = new_peak
            total_ref[pl.ds(hd, 1), :] = total
            acc_ref[hd] = acc

    own(0)
    for k in others:
        post(q_stage.at[k - 1], q_all.at[head], q_recv_sem.at[head], {"seq": seq, "head": lane(k)})
    own(1)
    own(2)
    hop(0, 1)
    own(3)
    hop(1, 1)
    partner()
    for k in range(1, classes):
        remote(
            q_stage.at[0], q_all.at[lane(k)], send_sem.at[0], q_recv_sem.at[lane(k)], across
        ).wait_recv()
    fold(0, 0, 0)
    hop(2, 1)
    fold(0, 0, 1)
    hop(3, 1)
    fold(0, 1, 0)
    partner_hop(1)
    waiting = [(0, 1, 1)]
    for t in range(1, depth):
        waiting += [(dz, dy, kind) for dy in (0, 1) for kind in (0, 1) for dz in (-t, t)]
        if t + 1 < depth:
            for k in range(classes):
                hop(k, t + 1)
                for item in waiting[:2]:
                    fold(*item)
                waiting = waiting[2:]
            partner_hop(t + 1)
    for item in waiting:
        fold(*item)
    for hd in range(heads_dev):
        done = acc_ref[hd] / total_ref[pl.ds(hd, 1), :]
        out_ref[:, hd * HEAD_DIM : (hd + 1) * HEAD_DIM] = done.T
    for *parts, when in pending:
        pl.when(when)(lambda parts=parts: remote(*parts).wait_send())


def gathered(queries, keys, values, random_blocks, global_blocks):
    seq_count, head_count = lax.axis_size("seq"), lax.axis_size("head")
    rows, width = queries.shape[0], queries.shape[1] // head_count
    heads_dev = width // HEAD_DIM
    tokens = rows * head_count
    rand_count, glob_count = random_blocks.shape[2], global_blocks.shape[0]
    dma = pltpu.SemaphoreType.DMA
    return pl.pallas_call(
        functools.partial(gathered_kernel, seq_count, head_count, rand_count, glob_count),
        out_shape=jax.ShapeDtypeStruct((tokens, width), jnp.float32),
        in_specs=[pl.BlockSpec(memory_space=pltpu.HBM)] * 4
        + [pl.BlockSpec(memory_space=pltpu.SMEM)],
        out_specs=pl.BlockSpec(memory_space=pltpu.VMEM),
        scratch_shapes=[
            pltpu.VMEM((seq_count * head_count, 2, rows, width), jnp.bfloat16),
            pltpu.VMEM(random_blocks.shape, jnp.int32),
            pltpu.VMEM((head_count, rows, width), jnp.bfloat16),
            pltpu.VMEM((head_count - 1, 2, rows, width), jnp.bfloat16),
            pltpu.VMEM((head_count - 1, rows, width), jnp.bfloat16),
            pltpu.VMEM((heads_dev * rand_count, tokens), jnp.int32),
            pltpu.VMEM((heads_dev, tokens), jnp.float32),
            pltpu.VMEM((heads_dev, tokens), jnp.float32),
            pltpu.VMEM((heads_dev, HEAD_DIM, tokens), jnp.float32),
            dma((3 * head_count + 1,)),
            dma((10 * seq_count + 24,)),
            dma((seq_count * head_count, 2)),
            dma((head_count,)),
        ],
        compiler_params=pltpu.CompilerParams(
            collective_id=0, has_side_effects=True
        ),
    )(queries, keys, values, random_blocks, global_blocks)


def shards(queries, keys, values, random_blocks, global_blocks):
    seq_count, head_count = lax.axis_size("seq"), lax.axis_size("head")
    pool_bytes = 4 * seq_count * queries.size
    fits = pool_bytes <= GATHER_LIMIT and queries.shape[0] == BLK
    if fits and head_count == 4 and seq_count % 2 == 0 and seq_count >= 6:
        return gathered(queries, keys, values, random_blocks, global_blocks)
    return exchanged(queries, keys, values, random_blocks, global_blocks)


def solution(mesh):
    in_specs = (
        P(("seq", "head"), None),
        P(("seq", "head"), None),
        P(("seq", "head"), None),
        P("seq", "head", None),
        P(),
    )
    out_specs = P("seq", "head")
    return jax.shard_map(shards, mesh=mesh, in_specs=in_specs, out_specs=out_specs, check_vma=False)
```
